1024 devices in a mesh: section: 32 (over z_hi, y, core), row: 4 (over x), col: 8 (over z_lo).
Axes of the slice: x: 4, y: 8, z: 16 (z_hi: 2, z_lo: 8; z = z_hi * 8 + z_lo), core: 2. Of those that a mesh axis runs over, the one named last changes fastest.
Arguments:
- weights: bfloat16 [32, 6144, 6144], P('section', ('row', 'col')), may hold values from -0.15625 to 0.15625
- acts: bfloat16 [32, 4, 6144, 128], P('section', None, ('row', 'col')), may hold values from -6 to 6
- grads: bfloat16 [32, 4, 6144, 128], P('section', None, ('row', 'col')), may hold values from -6 to 6
- saved: bfloat16 [32, 4, 6144, 128], P('section', None, ('row', 'col')), may hold values from -6 to 6
- plan: int32 [32, 2, 2], P('section'), may hold values from 0 to 3
Outputs:
- new_acts: bfloat16 [32, 4, 6144, 128], P('section', None, ('row', 'col'))
- new_grads: bfloat16 [32, 4, 6144, 128], P('section', None, ('row', 'col'))
The draws below stay inside these ranges and needn't reach their ends.
Inputs may be any that keep to these rules, and one draw needn't show every extreme that they name: plan[s, t, 0] is the slot read by section s's forward step in turn t and written by what arrives from section s - 1; plan[s, t, 1] likewise for the backward step and section s + 1.
All inputs are finite; a program needn't handle non-finite values.
Results may differ from the reference program's by a relative error of at most 0.017.
Values may be sent and summed in bfloat16 or wider, within the bound.
No kernel may reach another device: no remote copies, remote signals or barrier semaphores. Data moves between devices by JAX's collectives and lax.ppermute only.
A program may use at most 32 MiB of HBM per device.

```python
import jax
import jax.numpy as jnp
from jax import lax

D = 6144
MB = 128
SLOTS = 4
TICKS = 2
SECTIONS = 32
GRID = 32


def place_ends(result, own_key, smallest, high):
    index_at = [jax.random.randint(jax.random.fold_in(own_key, axis), (), 0, length) for axis, length in enumerate(result.shape)]
    longest = result.shape.index(max(result.shape))
    next_to = index_at[:longest] + [(index_at[longest] + 1) % result.shape[longest]] + index_at[longest + 1:]
    return result.at[tuple(index_at)].set(smallest).at[tuple(next_to)].set(high)


def with_spikes(drawn, stream_key, source, target, blocks, factor):
    owner, partner = [(jnp.arange(drawn.shape[position]) // (drawn.shape[position] // blocks)).reshape([-1 if axis == position else 1 for axis in range(drawn.ndim)]) for position in (source, target)]
    chosen = jax.random.permutation(stream_key, blocks)[partner]
    strong = (owner == chosen) | (owner == (partner + blocks // 2) % blocks)
    return jnp.where(strong, factor * drawn, drawn)


def level_of(own_key, shape, split, low, high):
    def one(dim, shards_of):
        heights = jax.random.uniform(jax.random.fold_in(jax.random.fold_in(own_key, 6), dim), (shards_of,), jnp.float32, low / len(split), high / len(split))
        return jnp.repeat(jnp.exp(heights), shape[dim] // shards_of).reshape((-1,) + (1,) * (len(shape) - dim - 1))

    loudness = one(*split[0])
    for cut in split[1:]:
        loudness = loudness * one(*cut)
    return loudness


def noise(rng, extent, spread, bound, shards=(), held_as=jnp.bfloat16):
    entries = jax.random.normal(rng, extent, jnp.float32) * spread
    if len(shards) > 0:
        entries = level_of(rng, extent, shards, -0.22, 0.18) * entries
    return jnp.clip(entries, min=-bound, max=bound).astype(held_as)


def gaussian_with(rng, extent, deviation, limit, cuts, heavy, kind=jnp.bfloat16):
    entries = deviation * jax.random.normal(rng, extent, jnp.float32)
    if cuts:
        entries = entries * level_of(rng, extent, cuts, -0.22, 0.18)
    return jnp.clip(with_spikes(entries, jax.random.fold_in(rng, 3), *heavy), -limit, limit).astype(kind)


def setup_inputs(seed: int = 0) -> dict:
    key_list = jax.random.split(jax.random.key(seed), 6)
    return {
        "weights": gaussian_with(key_list[0], (SECTIONS, D, D), D ** -0.5, 0.15625, ((0, 32), (1, 32)), (1, 2, 32, 2.75)),
        "acts": noise(key_list[1], (SECTIONS, SLOTS, D, MB), 1.0, 6.0, ((0, 32), (2, 32))),
        "grads": noise(key_list[2], (SECTIONS, SLOTS, D, MB), 1.0, 6.0, ((0, 32), (2, 32))),
        "saved": noise(key_list[3], (SECTIONS, SLOTS, D, MB), 1.0, 6.0, ((0, 32), (2, 32))),
        "plan": place_ends(jax.random.randint(key_list[4], (SECTIONS, TICKS, 2), 0, SLOTS), jax.random.fold_in(key_list[4], 1), 0, SLOTS - 1).astype(jnp.int32),
    }


def gelu_tanh(values):
    return jax.nn.gelu(values, approximate=True)

def forward_layer(paired):
    weight, inputs = paired
    grouped_weight = weight.reshape(GRID, D // GRID, D).astype(jnp.float32)
    grouped_inputs = inputs.reshape(GRID, D // GRID, MB).astype(jnp.float32)
    partial_value = jnp.einsum('gkn,gkm->gnm', grouped_weight, grouped_inputs).astype(jnp.bfloat16)
    partial_value = lax.optimization_barrier(partial_value)
    summed = lax.optimization_barrier(jnp.sum(partial_value.astype(jnp.float32), axis=0))
    return (inputs.astype(jnp.float32) + gelu_tanh(summed)).astype(jnp.bfloat16)

def backward_layer(tripled):
    weight, upstream, stored = tripled
    upstream_wide = upstream.astype(jnp.float32)
    slope_term = jax.vjp(gelu_tanh, stored.astype(jnp.float32))[1](upstream_wide)[0]
    scaled = slope_term.astype(jnp.bfloat16)
    carried = jnp.dot(weight, scaled, preferred_element_type=jnp.float32)
    return (upstream_wide + carried).astype(jnp.bfloat16)

def reference(weights, acts, grads, saved, plan):
    section_ids = jnp.arange(SECTIONS, dtype=jnp.int32)
    for turn_index in range(TICKS):
        front_slot = plan[:, turn_index, 0].astype(jnp.int32)
        back_slot = plan[:, turn_index, 1].astype(jnp.int32)
        inputs = acts[section_ids, front_slot]
        upstream = grads[section_ids, back_slot]
        stored = saved[section_ids, back_slot]
        outputs = lax.map(forward_layer, (weights, inputs))
        returned = lax.map(backward_layer, (weights, upstream, stored))
        acts = acts.at[section_ids, front_slot].set(jnp.roll(outputs, 1, axis=0))
        grads = grads.at[section_ids, back_slot].set(jnp.roll(returned, -1, axis=0))
    return (acts, grads)
```

```python
import jax
import jax.numpy as jnp
from jax import lax
from jax.sharding import PartitionSpec as P

TICKS = 2


def gelu_tanh(values):
    return jax.nn.gelu(values, approximate=True)


def paired(count, distance):
    return [(i, i ^ distance) for i in range(count)]


def shifted(block, axis, distance):
    count = lax.axis_size(axis)
    return lax.ppermute(block, axis, [((i - distance) % count, i) for i in range(count)])


def quads(count):
    return [list(range(i, i + 4)) for i in range(0, count, 4)]


def spread(pieces, axis):
    return lax.all_to_all(pieces, axis, 0, 0, tiled=True)


def spread_quad(pieces):
    count = lax.axis_size("col")
    return lax.all_to_all(
        pieces, "col", 0, 0, tiled=True, axis_index_groups=quads(count)
    )


def gather_col(block, upper):
    other = lax.ppermute(block, "col", paired(8, 4))
    low = jnp.where(upper, other, block)
    high = jnp.where(upper, block, other)
    pair = jnp.stack([low, high])
    got = spread_quad(jnp.broadcast_to(pair[None], (4, *pair.shape)))
    ordered = jnp.moveaxis(got, 0, 1)
    return ordered.reshape(8 * block.shape[0], block.shape[1])


def scatter_col(partial, upper):
    width = partial.shape[0] // 8
    blocks = partial.reshape(2, 4, width, partial.shape[1])
    got = spread_quad(jnp.moveaxis(blocks, 1, 0))
    pair = jnp.sum(got.astype(jnp.float32), axis=0)
    mine = jnp.where(upper, pair[1], pair[0])
    theirs = jnp.where(upper, pair[0], pair[1]).astype(jnp.bfloat16)
    return mine + lax.ppermute(theirs, "col", paired(8, 4)).astype(jnp.float32)


def swap_weight(weight):
    rows = lax.axis_size("row")
    place = lax.axis_index("row")
    width = weight.shape[1] // rows
    pieces = []
    for step in range(rows):
        piece = lax.dynamic_slice_in_dim(weight, (place ^ step) * width, width, 1)
        pieces.append(lax.ppermute(piece, "row", paired(rows, step)) if step else piece)
    return pieces


def in_row_order(pieces):
    place = lax.axis_index("row")
    whole = jnp.zeros((len(pieces), *pieces[0].shape), pieces[0].dtype)
    for step, piece in enumerate(pieces):
        whole = lax.dynamic_update_index_in_dim(whole, piece, place ^ step, 0)
    return whole


def shards(weights, acts, grads, saved, plan):
    weight = weights[0]
    held_inputs, held_grads, held_saved, table = acts[0], grads[0], saved[0], plan[0]
    width = weight.shape[0]
    upper = lax.axis_index("col") >= 4
    pieces = swap_weight(weight)
    for turn in range(TICKS):
        front, back = table[turn, 0], table[turn, 1]
        inputs = lax.dynamic_index_in_dim(held_inputs, front, 0, keepdims=False)
        upstream = lax.dynamic_index_in_dim(held_grads, back, 0, keepdims=False)
        stored = lax.dynamic_index_in_dim(held_saved, back, 0, keepdims=False)
        upstream_wide = upstream.astype(jnp.float32)
        slope = jax.vjp(gelu_tanh, stored.astype(jnp.float32))[1](upstream_wide)[0]
        slopes = gather_col(slope.astype(jnp.bfloat16), upper)
        gathered = spread(jnp.broadcast_to(inputs[None], (4, *inputs.shape)), "row")
        if turn == 0:
            slopes, gathered, pieces = lax.optimization_barrier((slopes, gathered, pieces))
            wide = in_row_order(pieces).reshape(-1, pieces[0].shape[1])
        partial = lax.dot_general(
            wide,
            gathered.reshape(-1, gathered.shape[2]),
            (((0,), (0,)), ((), ())),
            preferred_element_type=jnp.float32,
        ).astype(jnp.bfloat16)
        summed = scatter_col(partial, upper)
        outputs = (inputs.astype(jnp.float32) + gelu_tanh(summed)).astype(jnp.bfloat16)
        carried = jnp.dot(wide, slopes, preferred_element_type=jnp.float32).astype(jnp.bfloat16)
        back_parts = spread(carried.reshape(4, width, carried.shape[1]), "row")
        returned = (
            upstream_wide + jnp.sum(back_parts.astype(jnp.float32), axis=0)
        ).astype(jnp.bfloat16)
        arrived = shifted(outputs, "section", 1)
        sent_back = shifted(returned, "section", -1)
        held_inputs = lax.dynamic_update_index_in_dim(held_inputs, arrived, front, 0)
        held_grads = lax.dynamic_update_index_in_dim(held_grads, sent_back, back, 0)
    return (held_inputs[None], held_grads[None])


def solution(mesh):
    return jax.shard_map(
        shards,
        mesh=mesh,
        in_specs=(
            P("section", ("row", "col"), None),
            P("section", None, ("row", "col"), None),
            P("section", None, ("row", "col"), None),
            P("section", None, ("row", "col"), None),
            P("section", None, None),
        ),
        out_specs=(
            P("section", None, ("row", "col"), None),
            P("section", None, ("row", "col"), None),
        ),
        check_vma=False,
    )
```

```python
import jax
import jax.numpy as jnp
from jax import lax
from jax.sharding import PartitionSpec as P

ROWS = 4
COLS = 8
HALF = 16


def gelu_tanh(values):
    return jax.nn.gelu(values, approximate=True)


def paired(count, distance):
    return [(i, i ^ distance) for i in range(count)]


def quads(count):
    return [list(range(i, i + 4)) for i in range(0, count, 4)]


def is_far(section, step):
    return section % HALF == (HALF - 1 if step > 0 else 0)


def relay(block, step):
    count = lax.axis_size("section")
    route = []
    for section in range(count):
        twist = 4 if is_far(section, step) else 0
        for col in range(COLS):
            target = (section + step) % count
            route.append((section * COLS + col, target * COLS + (col ^ twist)))
    return lax.ppermute(block, ("section", "col"), route)


def twisted(block):
    count = lax.axis_size("section")
    route = []
    for section in range(HALF - 1, count, HALF):
        for col in range(COLS):
            route.append((section * COLS + col, section * COLS + (col ^ 4)))
    return lax.ppermute(block, ("section", "col"), route)


def permuted(block, axis, distance):
    return lax.ppermute(block, axis, paired(lax.axis_size(axis), distance))


def spread_row(pieces):
    return lax.all_to_all(pieces, "row", 0, 0, tiled=True)


def spread_quad(pieces):
    return lax.all_to_all(
        pieces, "col", 0, 0, tiled=True, axis_index_groups=quads(COLS)
    )


def slot_of(array, slot):
    return lax.dynamic_index_in_dim(array, slot, 0, keepdims=False, allow_negative_indices=False)


def with_slot(array, block, slot):
    return lax.dynamic_update_index_in_dim(array, block, slot, 0, allow_negative_indices=False)


def shards(weights, acts, grads, saved, plan):
    return turns(weights[0], acts[0], grads[0], saved[0], plan[0])


def quad_pieces(block, other, flipped):
    low = jnp.where(flipped, other, block)
    high = jnp.where(flipped, block, other)
    return jnp.broadcast_to(jnp.stack([low, high])[None], (4, 2, *block.shape))


def slope_of(upstream, stored):
    wide = upstream.astype(jnp.float32)
    return jax.vjp(gelu_tanh, stored.astype(jnp.float32))[1](wide)[0].astype(jnp.bfloat16)


def turns(weight, acts, grads, saved, table):
    width, tokens = acts.shape[1:]
    row, col, section = (lax.axis_index(a) for a in ("row", "col", "section"))
    upper = col >= 4
    ends = section % HALF == HALF - 1
    share = weight.shape[1] // ROWS
    wide = jnp.zeros((ROWS, width, share), weight.dtype)
    for step in range(ROWS):
        piece = lax.dynamic_slice(
            weight, (0, (row ^ step) * share), (width, share), allow_negative_indices=False
        )
        if step:
            piece = permuted(piece, "row", step)
        wide = with_slot(wide, piece, row ^ step)
    wide = wide.reshape(ROWS * width, share)
    front, back, later_front, later_back = (table[i, j] for i in (0, 1) for j in (0, 1))
    keep_high = upper ^ ends

    def forward_sums(x_row):
        sums = lax.dot_general(
            wide, x_row.reshape(-1, tokens), (((0,), (0,)), ((), ())),
            preferred_element_type=jnp.float32,
        ).astype(jnp.bfloat16)
        return jnp.moveaxis(sums.reshape(2, 4, width, tokens), 1, 0)

    def backward_sums(quad):
        slopes = jnp.moveaxis(quad, 0, 1).reshape(-1, tokens)
        sums = jnp.dot(wide, slopes, preferred_element_type=jnp.float32)
        return sums.astype(jnp.bfloat16).reshape(ROWS, width, tokens)

    def row_copies(block):
        return spread_row(jnp.broadcast_to(block[None], (ROWS, width, tokens)))

    def layer_output(got, residual):
        sums = jnp.sum(got.astype(jnp.float32), axis=0)
        kept = jnp.where(keep_high, sums[1], sums[0])
        sent = jnp.where(keep_high, sums[0], sums[1]).astype(jnp.bfloat16)
        summed = kept + permuted(sent, "col", 4).astype(jnp.float32)
        return (residual.astype(jnp.float32) + gelu_tanh(summed)).astype(jnp.bfloat16)

    def input_gradient(carried, upstream):
        parts = spread_row(carried).astype(jnp.float32)
        return (upstream.astype(jnp.float32) + jnp.sum(parts, axis=0)).astype(jnp.bfloat16)

    inputs = slot_of(acts, front)
    upstream = slot_of(grads, back)
    slope = slope_of(upstream, slot_of(saved, back))
    other = permuted(slope, "col", 4)
    x_row = row_copies(inputs)
    quad = spread_quad(quad_pieces(slope, other, upper))
    residual = jnp.where(ends, twisted(inputs), inputs)
    ahead = jnp.stack([slot_of(grads, later_back), slot_of(saved, later_back)])
    ahead = jnp.where(ends, twisted(ahead), ahead)

    returned = input_gradient(backward_sums(quad), upstream)
    returned = relay(returned, -1)
    got = spread_quad(forward_sums(x_row))
    arrived = relay(layer_output(got, residual), 1)

    same_front = later_front == front
    same_back = later_back == back
    slope = slope_of(jnp.where(same_back, returned, ahead[0]), ahead[1])
    other = permuted(slope, "col", 4)
    inputs = jnp.where(same_front, arrived, slot_of(acts, later_front))
    x_row = row_copies(inputs)
    residual = jnp.where(ends, twisted(inputs), inputs)
    fixed = jnp.where(ends, twisted(returned), returned)
    upstream = jnp.where(same_back, fixed, slot_of(grads, later_back))
    both = jnp.concatenate(
        [forward_sums(x_row), quad_pieces(slope, other, keep_high)], axis=1
    )
    both = spread_quad(both)
    held_inputs, held_grads = lax.optimization_barrier((acts, grads))
    held_inputs = with_slot(held_inputs, arrived, front)
    held_grads = with_slot(held_grads, fixed, back)
    returned = input_gradient(backward_sums(both[:, 2:]), upstream)
    returned = relay(returned, -1)
    arrived = relay(layer_output(both[:, :2], residual), 1)
    fixed = jnp.where(ends, twisted(returned), returned)
    held_inputs = with_slot(held_inputs, arrived, later_front)
    held_grads = with_slot(held_grads, fixed, later_back)
    return (held_inputs[None], held_grads[None])


def solution(mesh):
    return jax.shard_map(
        shards,
        mesh=mesh,
        in_specs=(
            P("section", ("row", "col"), None),
            P("section", None, ("row", "col"), None),
            P("section", None, ("row", "col"), None),
            P("section", None, ("row", "col"), None),
            P("section", None, None),
        ),
        out_specs=(
            P("section", None, ("row", "col"), None),
            P("section", None, ("row", "col"), None),
        ),
        check_vma=False,
    )
```

```python
import jax
import jax.numpy as jnp
from jax import lax
from jax.sharding import PartitionSpec as P

ROWS = 4
COLS = 8
HALF = 16
SLOTS = 4


def gelu_tanh(values):
    return jax.nn.gelu(values, approximate=True)


def paired(count, distance):
    return [(i, i ^ distance) for i in range(count)]


def quads(count):
    return [list(range(i, i + 4)) for i in range(0, count, 4)]


def is_far(section, step):
    return section % HALF == (HALF - 1 if step > 0 else 0)


def relay(block, step):
    count = lax.axis_size("section")
    route = []
    for section in range(count):
        twist = 4 if is_far(section, step) else 0
        for col in range(COLS):
            target = (section + step) % count
            route.append((section * COLS + col, target * COLS + (col ^ twist)))
    return lax.ppermute(block, ("section", "col"), route)


def twisted(block):
    count = lax.axis_size("section")
    route = []
    for section in range(HALF - 1, count, HALF):
        for col in range(COLS):
            route.append((section * COLS + col, section * COLS + (col ^ 4)))
    return lax.ppermute(block, ("section", "col"), route)


def permuted(block, axis, distance):
    return lax.ppermute(block, axis, paired(lax.axis_size(axis), distance))


def spread_row(pieces):
    return lax.all_to_all(pieces, "row", 0, 0, tiled=True)


def spread_quad(pieces):
    return lax.all_to_all(
        pieces, "col", 0, 0, tiled=True, axis_index_groups=quads(COLS)
    )


def slot_of(array, slot):
    return lax.dynamic_index_in_dim(array, slot, 0, keepdims=False, allow_negative_indices=False)


def with_slot(array, block, slot):
    return lax.dynamic_update_index_in_dim(array, block, slot, 0, allow_negative_indices=False)


def shards(weights, acts, grads, saved, plan):
    return turns(weights[0], acts[0], grads[0], saved[0], plan[0])


def quad_pieces(block, other, flipped):
    low = jnp.where(flipped, other, block)
    high = jnp.where(flipped, block, other)
    return jnp.broadcast_to(jnp.stack([low, high])[None], (4, 2, *block.shape))


def slope_of(upstream, stored):
    wide = upstream.astype(jnp.float32)
    return jax.vjp(gelu_tanh, stored.astype(jnp.float32))[1](wide)[0].astype(jnp.bfloat16)


def turns(weight, acts, grads, saved, table):
    width, tokens = acts.shape[1:]
    row, col, section = (lax.axis_index(a) for a in ("row", "col", "section"))
    upper = col >= 4
    ends = (section & (HALF - 1)) == HALF - 1
    share = weight.shape[1] // ROWS
    wide = jnp.zeros((ROWS, width, share), weight.dtype)
    for step in range(ROWS):
        piece = lax.dynamic_slice(
            weight, (0, (row ^ step) * share), (width, share), allow_negative_indices=False
        )
        if step:
            piece = permuted(piece, "row", step)
        wide = with_slot(wide, piece, row ^ step)
    wide = wide.reshape(ROWS * width, share)
    front, back, later_front, later_back = (
        jnp.where(table[i, j] < 0, table[i, j] + SLOTS, table[i, j])
        for i in (0, 1)
        for j in (0, 1)
    )
    keep_high = upper ^ ends
    same_front = later_front == front
    same_back = later_back == back

    def forward_sums(x_row):
        sums = lax.dot_general(
            wide, x_row.reshape(-1, tokens), (((0,), (0,)), ((), ())),
            preferred_element_type=jnp.float32,
        ).astype(jnp.bfloat16)
        return jnp.moveaxis(sums.reshape(2, 4, width, tokens), 1, 0)

    def backward_sums(quad):
        slopes = jnp.moveaxis(quad, 0, 1).reshape(-1, tokens)
        sums = jnp.dot(wide, slopes, preferred_element_type=jnp.float32)
        return sums.astype(jnp.bfloat16).reshape(ROWS, width, tokens)

    def row_copies(block):
        return spread_row(jnp.broadcast_to(block[None], (ROWS, width, tokens)))

    def layer_output(got, residual):
        sums = jnp.sum(got.astype(jnp.float32), axis=0)
        kept = jnp.where(keep_high, sums[1], sums[0])
        sent = jnp.where(keep_high, sums[0], sums[1]).astype(jnp.bfloat16)
        summed = kept + permuted(sent, "col", 4).astype(jnp.float32)
        return (residual.astype(jnp.float32) + gelu_tanh(summed)).astype(jnp.bfloat16)

    def input_gradient(carried, upstream):
        parts = spread_row(carried).astype(jnp.float32)
        return (upstream.astype(jnp.float32) + jnp.sum(parts, axis=0)).astype(jnp.bfloat16)

    inputs = slot_of(acts, front)
    upstream = slot_of(grads, back)
    slope = slope_of(upstream, slot_of(saved, back))
    other = permuted(slope, "col", 4)
    other, ends, keep_high, same_front, same_back, later_front = lax.optimization_barrier(
        (other, ends, keep_high, same_front, same_back, later_front)
    )
    x_row = row_copies(inputs)
    pair = jnp.stack([jnp.where(upper, other, slope), jnp.where(upper, slope, other)])
    quad = jnp.zeros((4, *pair.shape), pair.dtype)
    for step in range(4):
        block = permuted(pair, "col", step) if step else pair
        quad = with_slot(quad, block, (col & 3) ^ step)
    residual = jnp.where(ends, twisted(inputs), inputs)
    ahead = jnp.stack([slot_of(grads, later_back), slot_of(saved, later_back)])
    ahead = jnp.where(ends, twisted(ahead), ahead)

    returned = input_gradient(backward_sums(quad), upstream)
    returned = relay(returned, -1)
    got = spread_quad(forward_sums(x_row))
    arrived = relay(layer_output(got, residual), 1)

    slope = slope_of(jnp.where(same_back, returned, ahead[0]), ahead[1])
    other = permuted(slope, "col", 4)
    inputs = jnp.where(same_front, arrived, slot_of(acts, later_front))
    x_row = row_copies(inputs)
    residual = jnp.where(ends, twisted(inputs), inputs)
    fixed = jnp.where(ends, twisted(returned), returned)
    upstream = jnp.where(same_back, fixed, slot_of(grads, later_back))
    both = jnp.concatenate(
        [forward_sums(x_row), quad_pieces(slope, other, keep_high)], axis=1
    )
    both = spread_quad(both)
    held_inputs, held_grads = lax.optimization_barrier((acts, grads))
    held_inputs = with_slot(held_inputs, arrived, front)
    held_grads = with_slot(held_grads, fixed, back)
    returned = input_gradient(backward_sums(both[:, 2:]), upstream)
    returned = relay(returned, -1)
    arrived = relay(layer_output(both[:, :2], residual), 1)
    fixed = jnp.where(ends, twisted(returned), returned)
    held_inputs = with_slot(held_inputs, arrived, later_front)
    held_grads = with_slot(held_grads, fixed, later_back)
    return (held_inputs[None], held_grads[None])


def solution(mesh):
    return jax.shard_map(
        shards,
        mesh=mesh,
        in_specs=(
            P("section", ("row", "col"), None),
            P("section", None, ("row", "col"), None),
            P("section", None, ("row", "col"), None),
            P("section", None, ("row", "col"), None),
            P("section", None, None),
        ),
        out_specs=(
            P("section", None, ("row", "col"), None),
            P("section", None, ("row", "col"), None),
        ),
        check_vma=False,
    )
```

```python
import jax
import jax.numpy as jnp
from jax import lax
from jax.sharding import PartitionSpec as P

ROWS = 4
COLS = 8
HALF = 16
SLOTS = 4


def gelu_tanh(values):
    return jax.nn.gelu(values, approximate=True)


def paired(count, distance):
    return [(i, i ^ distance) for i in range(count)]


def quads(count):
    return [list(range(i, i + 4)) for i in range(0, count, 4)]


def relay(block, step):
    count = lax.axis_size("section")
    route = []
    for section in range(count):
        twist = 4 if step > 0 and section % HALF == HALF - 1 else 0
        for col in range(COLS):
            target = (section + step) % count
            route.append((section * COLS + col, target * COLS + (col ^ twist)))
    return lax.ppermute(block, ("section", "col"), route)


def twisted(block):
    count = lax.axis_size("section")
    route = []
    for section in range(HALF - 1, count, HALF):
        for col in range(COLS):
            route.append((section * COLS + col, section * COLS + (col ^ 4)))
    return lax.ppermute(block, ("section", "col"), route)


def permuted(block, axis, distance):
    return lax.ppermute(block, axis, paired(lax.axis_size(axis), distance))


def spread_row(pieces):
    return lax.all_to_all(pieces, "row", 0, 0, tiled=True)


def spread_quad(pieces):
    return lax.all_to_all(
        pieces, "col", 0, 0, tiled=True, axis_index_groups=quads(COLS)
    )


def slot_of(array, slot):
    return lax.dynamic_index_in_dim(array, slot, 0, keepdims=False, allow_negative_indices=False)


def with_slot(array, block, slot):
    return lax.dynamic_update_index_in_dim(array, block, slot, 0, allow_negative_indices=False)


def shards(weights, acts, grads, saved, plan):
    return turns(weights[0], acts[0], grads[0], saved[0], plan[0])


def quad_pieces(block, other, flipped):
    low = jnp.where(flipped, other, block)
    high = jnp.where(flipped, block, other)
    return jnp.broadcast_to(jnp.stack([low, high])[None], (4, 2, *block.shape))


def slope_of(upstream, stored):
    wide = upstream.astype(jnp.float32)
    return jax.vjp(gelu_tanh, stored.astype(jnp.float32))[1](wide)[0].astype(jnp.bfloat16)


def turns(weight, acts, grads, saved, table):
    width, tokens = acts.shape[1:]
    row, col, section = (lax.axis_index(a) for a in ("row", "col", "section"))
    upper = col >= 4
    ends = (section & (HALF - 1)) == HALF - 1
    share = weight.shape[1] // ROWS
    front, back, later_front, later_back = (
        jnp.where(table[i, j] < 0, table[i, j] + SLOTS, table[i, j])
        for i in (0, 1)
        for j in (0, 1)
    )
    inputs = slot_of(acts, front)
    wide = jnp.zeros((ROWS, width, share), weight.dtype)
    x_row = jnp.zeros((ROWS, width, tokens), acts.dtype)
    for step in range(ROWS):
        piece = lax.dynamic_slice(
            weight, (0, (row ^ step) * share), (width, share), allow_negative_indices=False
        )
        block = inputs
        if step:
            piece = jnp.concatenate([piece, inputs], axis=1)
            piece = permuted(piece, "row", step)
            piece, block = piece[:, :share], piece[:, share:]
        wide = with_slot(wide, piece, row ^ step)
        x_row = with_slot(x_row, block, row ^ step)
    wide = wide.reshape(ROWS * width, share)
    keep_high = upper ^ ends
    same_front = later_front == front
    same_back = later_back == back

    def forward_sums(x_row):
        sums = lax.dot_general(
            wide, x_row.reshape(-1, tokens), (((0,), (0,)), ((), ())),
            preferred_element_type=jnp.float32,
        ).astype(jnp.bfloat16)
        return jnp.moveaxis(sums.reshape(2, 4, width, tokens), 1, 0)

    def backward_sums(quad):
        slopes = jnp.moveaxis(quad, 0, 1).reshape(-1, tokens)
        sums = jnp.dot(wide, slopes, preferred_element_type=jnp.float32)
        return sums.astype(jnp.bfloat16).reshape(ROWS, width, tokens)

    def row_copies(block):
        return spread_row(jnp.broadcast_to(block[None], (ROWS, width, tokens)))

    def layer_output(got, residual):
        sums = jnp.sum(got.astype(jnp.float32), axis=0)
        kept = jnp.where(keep_high, sums[1], sums[0])
        sent = jnp.where(keep_high, sums[0], sums[1]).astype(jnp.bfloat16)
        summed = kept + permuted(sent, "col", 4).astype(jnp.float32)
        return (residual.astype(jnp.float32) + gelu_tanh(summed)).astype(jnp.bfloat16)

    def input_gradient(carried, upstream):
        parts = spread_row(carried).astype(jnp.float32)
        return (upstream.astype(jnp.float32) + jnp.sum(parts, axis=0)).astype(jnp.bfloat16)

    upstream = slot_of(grads, back)
    slope = slope_of(upstream, slot_of(saved, back))
    other = permuted(slope, "col", 4)
    other, ends, keep_high, same_front, same_back, later_front = lax.optimization_barrier(
        (other, ends, keep_high, same_front, same_back, later_front)
    )
    quad = spread_quad(quad_pieces(slope, other, upper))
    residual = jnp.where(ends, twisted(inputs), inputs)
    got = spread_quad(forward_sums(x_row))
    returned = input_gradient(backward_sums(quad), upstream)
    arrived = relay(layer_output(got, residual), 1)
    returned = relay(returned, -1)

    inputs = jnp.where(same_front, arrived, slot_of(acts, later_front))
    x_row = row_copies(inputs)
    residual = jnp.where(ends, twisted(inputs), inputs)
    upstream = jnp.where(same_back, returned, slot_of(grads, later_back))
    slope = slope_of(upstream, slot_of(saved, later_back))
    other = permuted(slope, "col", 4)
    both = jnp.concatenate([forward_sums(x_row), quad_pieces(slope, other, upper)], axis=1)
    both = spread_quad(both)
    held_inputs, held_grads = lax.optimization_barrier((acts, grads))
    held_inputs = with_slot(held_inputs, arrived, front)
    held_grads = with_slot(held_grads, returned, back)
    returned = input_gradient(backward_sums(both[:, 2:]), upstream)
    returned = relay(returned, -1)
    arrived = relay(layer_output(both[:, :2], residual), 1)
    held_inputs = with_slot(held_inputs, arrived, later_front)
    held_grads = with_slot(held_grads, returned, later_back)
    return (held_inputs[None], held_grads[None])


def solution(mesh):
    return jax.shard_map(
        shards,
        mesh=mesh,
        in_specs=(
            P("section", ("row", "col"), None),
            P("section", None, ("row", "col"), None),
            P("section", None, ("row", "col"), None),
            P("section", None, ("row", "col"), None),
            P("section", None, None),
        ),
        out_specs=(
            P("section", None, ("row", "col"), None),
            P("section", None, ("row", "col"), None),
        ),
        check_vma=False,
    )
```

```python
import jax
import jax.numpy as jnp
from jax import lax
from jax.sharding import PartitionSpec as P

ROWS = 4
COLS = 8
HALF = 16
SLOTS = 4
ARRIVAL = (0, 2, 1, 3)


def gelu_tanh(values):
    return jax.nn.gelu(values, approximate=True)


def paired(count, distance):
    return [(i, i ^ distance) for i in range(count)]


def quads(count):
    return [list(range(i, i + 4)) for i in range(0, count, 4)]


def relay(block, step):
    count = lax.axis_size("section")
    route = []
    for section in range(count):
        twist = 4 if step > 0 and section % HALF == HALF - 1 else 0
        for col in range(COLS):
            target = (section + step) % count
            route.append((section * COLS + col, target * COLS + (col ^ twist)))
    return lax.ppermute(block, ("section", "col"), route)


def twisted(block):
    count = lax.axis_size("section")
    route = []
    for section in range(HALF - 1, count, HALF):
        for col in range(COLS):
            route.append((section * COLS + col, section * COLS + (col ^ 4)))
    return lax.ppermute(block, ("section", "col"), route)


def permuted(block, axis, distance):
    return lax.ppermute(block, axis, paired(lax.axis_size(axis), distance))


def from_row(block):
    return [block] + [permuted(block, "row", k) for k in range(1, ROWS)]


def spread_quad(pieces):
    return lax.all_to_all(
        pieces, "col", 0, 0, tiled=True, axis_index_groups=quads(COLS)
    )


def slot_of(array, slot):
    return lax.dynamic_index_in_dim(array, slot, 0, keepdims=False, allow_negative_indices=False)


def with_slot(array, block, slot):
    return lax.dynamic_update_index_in_dim(array, block, slot, 0, allow_negative_indices=False)


def shards(weights, acts, grads, saved, plan):
    return turns(weights[0], acts[0], grads[0], saved[0], plan[0])


def quad_pieces(block, other, flipped):
    low = jnp.where(flipped, other, block)
    high = jnp.where(flipped, block, other)
    return jnp.broadcast_to(jnp.stack([low, high])[None], (4, 2, *block.shape))


def slope_of(upstream, stored):
    wide = upstream.astype(jnp.float32)
    return jax.vjp(gelu_tanh, stored.astype(jnp.float32))[1](wide)[0].astype(jnp.bfloat16)


def turns(weight, acts, grads, saved, table):
    width, tokens = acts.shape[1:]
    row, col, section = (lax.axis_index(a) for a in ("row", "col", "section"))
    upper = col >= 4
    ends = (section & (HALF - 1)) == HALF - 1
    share = weight.shape[1] // ROWS
    front, back, later_front, later_back = (
        jnp.where(table[i, j] < 0, table[i, j] + SLOTS, table[i, j])
        for i in (0, 1)
        for j in (0, 1)
    )
    pieces = []
    for step in range(ROWS):
        piece = lax.dynamic_slice(
            weight, (0, (row ^ step) * share), (width, share), allow_negative_indices=False
        )
        pieces.append(permuted(piece, "row", step) if step else piece)
    keep_high = upper ^ ends
    same_front = later_front == front
    same_back = later_back == back

    def forward_sums(blocks):
        sums = 0.0
        for step in ARRIVAL:
            sums = sums + lax.dot_general(
                pieces[step], blocks[step], (((0,), (0,)), ((), ())),
                preferred_element_type=jnp.float32,
            )
        sums = sums.astype(jnp.bfloat16)
        return jnp.moveaxis(sums.reshape(2, 4, width, tokens), 1, 0)

    def layer_output(got, residual):
        sums = jnp.sum(got.astype(jnp.float32), axis=0)
        kept = jnp.where(keep_high, sums[1], sums[0])
        sent = jnp.where(keep_high, sums[0], sums[1]).astype(jnp.bfloat16)
        summed = kept + permuted(sent, "col", 4).astype(jnp.float32)
        return (residual.astype(jnp.float32) + gelu_tanh(summed)).astype(jnp.bfloat16)

    def input_gradient(quad, upstream):
        slopes = jnp.moveaxis(quad, 0, 1).reshape(-1, tokens)
        total = upstream.astype(jnp.float32)
        for step, piece in enumerate(pieces):
            part = jnp.dot(piece, slopes, preferred_element_type=jnp.float32)
            if step:
                part = permuted(part.astype(jnp.bfloat16), "row", step)
            total = total + part.astype(jnp.float32)
        return total.astype(jnp.bfloat16)

    inputs = slot_of(acts, front)
    upstream = slot_of(grads, back)
    slope = slope_of(upstream, slot_of(saved, back))
    other = permuted(slope, "col", 4)
    later_inputs = slot_of(acts, later_front)
    later_upstream = slot_of(grads, later_back)
    later_stored = slot_of(saved, later_back)
    other, ends, keep_high, same_front, same_back, later_front = lax.optimization_barrier(
        (other, ends, keep_high, same_front, same_back, later_front)
    )
    later_inputs, later_upstream, later_stored, other = lax.optimization_barrier(
        (later_inputs, later_upstream, later_stored, other)
    )
    blocks = from_row(inputs)
    quad = spread_quad(quad_pieces(slope, other, upper))
    residual = jnp.where(ends, twisted(inputs), inputs)
    got = spread_quad(forward_sums(blocks))
    returned = relay(input_gradient(quad, upstream), -1)
    arrived = relay(layer_output(got, residual), 1)

    inputs = jnp.where(same_front, arrived, later_inputs)
    blocks = from_row(inputs)
    residual = jnp.where(ends, twisted(inputs), inputs)
    upstream = jnp.where(same_back, returned, later_upstream)
    slope = slope_of(upstream, later_stored)
    other = permuted(slope, "col", 4)
    both = jnp.concatenate([forward_sums(blocks), quad_pieces(slope, other, upper)], axis=1)
    both = spread_quad(both)
    held_inputs, held_grads, both = lax.optimization_barrier((acts, grads, both))
    held_inputs = with_slot(held_inputs, arrived, front)
    held_grads = with_slot(held_grads, returned, back)
    returned = input_gradient(both[:, 2:], upstream)
    returned = relay(returned, -1)
    arrived = relay(layer_output(both[:, :2], residual), 1)
    held_inputs = with_slot(held_inputs, arrived, later_front)
    held_grads = with_slot(held_grads, returned, later_back)
    return (held_inputs[None], held_grads[None])


def solution(mesh):
    return jax.shard_map(
        shards,
        mesh=mesh,
        in_specs=(
            P("section", ("row", "col"), None),
            P("section", None, ("row", "col"), None),
            P("section", None, ("row", "col"), None),
            P("section", None, ("row", "col"), None),
            P("section", None, None),
        ),
        out_specs=(
            P("section", None, ("row", "col"), None),
            P("section", None, ("row", "col"), None),
        ),
        check_vma=False,
    )
```

```python
import jax
import jax.numpy as jnp
from jax import lax
from jax.sharding import PartitionSpec as P

ROWS = 4
COLS = 8
HALF = 16
SLOTS = 4
ARRIVAL = (0, 2, 1, 3)


def gelu_tanh(values):
    return jax.nn.gelu(values, approximate=True)


def paired(count, distance):
    return [(i, i ^ distance) for i in range(count)]


def quads(count):
    return [list(range(i, i + 4)) for i in range(0, count, 4)]


def relay(block, step):
    count = lax.axis_size("section")
    route = []
    for section in range(count):
        twist = 4 if step > 0 and section % HALF == HALF - 1 else 0
        for col in range(COLS):
            target = (section + step) % count
            route.append((section * COLS + col, target * COLS + (col ^ twist)))
    return lax.ppermute(block, ("section", "col"), route)


def twisted(block):
    count = lax.axis_size("section")
    route = []
    for section in range(HALF - 1, count, HALF):
        for col in range(COLS):
            route.append((section * COLS + col, section * COLS + (col ^ 4)))
    return lax.ppermute(block, ("section", "col"), route)


def permuted(block, axis, distance):
    return lax.ppermute(block, axis, paired(lax.axis_size(axis), distance))


def from_row(block):
    return [block] + [permuted(block, "row", k) for k in range(1, ROWS)]


def spread_row(pieces):
    return lax.all_to_all(pieces, "row", 0, 0, tiled=True)


def spread_quad(pieces):
    return lax.all_to_all(
        pieces, "col", 0, 0, tiled=True, axis_index_groups=quads(COLS)
    )


def slot_of(array, slot):
    return lax.dynamic_index_in_dim(array, slot, 0, keepdims=False, allow_negative_indices=False)


def with_slot(array, block, slot):
    return lax.dynamic_update_index_in_dim(array, block, slot, 0, allow_negative_indices=False)


def shards(weights, acts, grads, saved, plan):
    return turns(weights[0], acts[0], grads[0], saved[0], plan[0])


def quad_pieces(block, other, flipped):
    low = jnp.where(flipped, other, block)
    high = jnp.where(flipped, block, other)
    return jnp.broadcast_to(jnp.stack([low, high])[None], (4, 2, *block.shape))


def slope_of(upstream, stored):
    wide = upstream.astype(jnp.float32)
    return jax.vjp(gelu_tanh, stored.astype(jnp.float32))[1](wide)[0].astype(jnp.bfloat16)


def turns(weight, acts, grads, saved, table):
    width, tokens = acts.shape[1:]
    row, col, section = (lax.axis_index(a) for a in ("row", "col", "section"))
    upper = col >= 4
    ends = (section & (HALF - 1)) == HALF - 1
    share = weight.shape[1] // ROWS
    front, back, later_front, later_back = (
        jnp.where(table[i, j] < 0, table[i, j] + SLOTS, table[i, j])
        for i in (0, 1)
        for j in (0, 1)
    )
    pieces = []
    for step in range(ROWS):
        piece = lax.dynamic_slice(
            weight, (0, (row ^ step) * share), (width, share), allow_negative_indices=False
        )
        pieces.append(permuted(piece, "row", step) if step else piece)
    keep_high = upper ^ ends
    same_front = later_front == front
    same_back = later_back == back

    def forward_sums(blocks):
        sums = 0.0
        for step in ARRIVAL:
            sums = sums + lax.dot_general(
                pieces[step], blocks[step], (((0,), (0,)), ((), ())),
                preferred_element_type=jnp.float32,
            )
        sums = sums.astype(jnp.bfloat16)
        return jnp.moveaxis(sums.reshape(2, 4, width, tokens), 1, 0)

    def layer_output(got, residual):
        sums = jnp.sum(got.astype(jnp.float32), axis=0)
        kept = jnp.where(keep_high, sums[1], sums[0])
        sent = jnp.where(keep_high, sums[0], sums[1]).astype(jnp.bfloat16)
        summed = kept + permuted(sent, "col", 4).astype(jnp.float32)
        return (residual.astype(jnp.float32) + gelu_tanh(summed)).astype(jnp.bfloat16)

    def input_gradient(quad, upstream):
        slopes = jnp.moveaxis(quad, 0, 1).reshape(-1, tokens)
        parts = jnp.zeros((ROWS, width, tokens), jnp.bfloat16)
        for step, piece in enumerate(pieces):
            part = jnp.dot(piece, slopes, preferred_element_type=jnp.float32)
            parts = with_slot(parts, part.astype(jnp.bfloat16), row ^ step)
        parts = spread_row(parts).astype(jnp.float32)
        return (upstream.astype(jnp.float32) + jnp.sum(parts, axis=0)).astype(jnp.bfloat16)

    inputs = slot_of(acts, front)
    upstream = slot_of(grads, back)
    slope = slope_of(upstream, slot_of(saved, back))
    other = permuted(slope, "col", 4)
    later_inputs = slot_of(acts, later_front)
    later_upstream = slot_of(grads, later_back)
    later_stored = slot_of(saved, later_back)
    other, ends, keep_high, same_front, same_back, later_front = lax.optimization_barrier(
        (other, ends, keep_high, same_front, same_back, later_front)
    )
    later_inputs, later_upstream, later_stored, other = lax.optimization_barrier(
        (later_inputs, later_upstream, later_stored, other)
    )
    blocks = from_row(inputs)
    quad = spread_quad(quad_pieces(slope, other, upper))
    residual = jnp.where(ends, twisted(inputs), inputs)
    got = spread_quad(forward_sums(blocks))
    returned = relay(input_gradient(quad, upstream), -1)
    arrived = relay(layer_output(got, residual), 1)

    inputs = jnp.where(same_front, arrived, later_inputs)
    copies = jnp.broadcast_to(inputs[None], (ROWS, width, tokens))
    copies = spread_row(copies)
    blocks = [slot_of(copies, row ^ step) for step in range(ROWS)]
    residual = jnp.where(ends, twisted(inputs), inputs)
    upstream = jnp.where(same_back, returned, later_upstream)
    slope = slope_of(upstream, later_stored)
    other = permuted(slope, "col", 4)
    both = jnp.concatenate([forward_sums(blocks), quad_pieces(slope, other, upper)], axis=1)
    both = spread_quad(both)
    slots = jnp.arange(SLOTS)[:, None, None]
    held_inputs = jnp.where(slots == front, arrived, acts)
    held_grads = jnp.where(slots == back, returned, grads)
    returned = input_gradient(both[:, 2:], upstream)
    returned = relay(returned, -1)
    arrived = relay(layer_output(both[:, :2], residual), 1)
    held_inputs = jnp.where(slots == later_front, arrived, held_inputs)
    held_grads = jnp.where(slots == later_back, returned, held_grads)
    return (held_inputs[None], held_grads[None])


def solution(mesh):
    return jax.shard_map(
        shards,
        mesh=mesh,
        in_specs=(
            P("section", ("row", "col"), None),
            P("section", None, ("row", "col"), None),
            P("section", None, ("row", "col"), None),
            P("section", None, ("row", "col"), None),
            P("section", None, None),
        ),
        out_specs=(
            P("section", None, ("row", "col"), None),
            P("section", None, ("row", "col"), None),
        ),
        check_vma=False,
    )
```

```python
import jax
import jax.numpy as jnp
from jax import lax
from jax.sharding import PartitionSpec as P

ROWS = 4
COLS = 8
HALF = 16
SLOTS = 4
ARRIVAL = (0, 2, 1, 3)


def gelu_tanh(values):
    return jax.nn.gelu(values, approximate=True)


def paired(count, distance):
    return [(i, i ^ distance) for i in range(count)]


def quads(count):
    return [list(range(i, i + 4)) for i in range(0, count, 4)]


def relay(block, step, senders=None):
    count = lax.axis_size("section")
    route = []
    for section in range(count) if senders is None else senders:
        twist = 4 if step > 0 and section % HALF == HALF - 1 else 0
        for col in range(COLS):
            target = (section + step) % count
            route.append((section * COLS + col, target * COLS + (col ^ twist)))
    return lax.ppermute(block, ("section", "col"), route)


def twisted(block):
    count = lax.axis_size("section")
    route = []
    for section in range(HALF - 1, count, HALF):
        for col in range(COLS):
            route.append((section * COLS + col, section * COLS + (col ^ 4)))
    return lax.ppermute(block, ("section", "col"), route)


def permuted(block, axis, distance):
    return lax.ppermute(block, axis, paired(lax.axis_size(axis), distance))


def from_row(block):
    return [block] + [permuted(block, "row", k) for k in range(1, ROWS)]


def spread_row(pieces):
    return lax.all_to_all(pieces, "row", 0, 0, tiled=True)


def spread_quad(pieces):
    return lax.all_to_all(
        pieces, "col", 0, 0, tiled=True, axis_index_groups=quads(COLS)
    )


def slot_of(array, slot):
    return lax.dynamic_index_in_dim(array, slot, 0, keepdims=False, allow_negative_indices=False)


def with_slot(array, block, slot):
    return lax.dynamic_update_index_in_dim(array, block, slot, 0, allow_negative_indices=False)


def shards(weights, acts, grads, saved, plan):
    return turns(weights[0], acts[0], grads[0], saved[0], plan[0])


def quad_pieces(block, other, flipped):
    low = jnp.where(flipped, other, block)
    high = jnp.where(flipped, block, other)
    return jnp.broadcast_to(jnp.stack([low, high])[None], (4, 2, *block.shape))


def slope_of(upstream, stored):
    wide = upstream.astype(jnp.float32)
    return jax.vjp(gelu_tanh, stored.astype(jnp.float32))[1](wide)[0].astype(jnp.bfloat16)


def turns(weight, acts, grads, saved, table):
    width, tokens = acts.shape[1:]
    row, col, section = (lax.axis_index(a) for a in ("row", "col", "section"))
    upper = col >= 4
    ends = (section & (HALF - 1)) == HALF - 1
    share = weight.shape[1] // ROWS
    front, back, later_front, later_back = (
        jnp.where(table[i, j] < 0, table[i, j] + SLOTS, table[i, j])
        for i in (0, 1)
        for j in (0, 1)
    )
    pieces = []
    for step in range(ROWS):
        piece = lax.dynamic_slice(
            weight, (0, (row ^ step) * share), (width, share), allow_negative_indices=False
        )
        if step:
            pieces.append(permuted(piece, "row", step))
        else:
            pieces.append(lax.optimization_barrier(piece))
    keep_high = upper ^ ends
    same_front = later_front == front
    same_back = later_back == back

    def forward_sums(blocks):
        sums = 0.0
        for step in ARRIVAL:
            sums = sums + lax.dot_general(
                pieces[step], blocks[step], (((0,), (0,)), ((), ())),
                preferred_element_type=jnp.float32,
            )
        sums = sums.astype(jnp.bfloat16)
        return jnp.moveaxis(sums.reshape(2, 4, width, tokens), 1, 0)

    def layer_output(got, residual):
        sums = jnp.sum(got.astype(jnp.float32), axis=0)
        kept = jnp.where(keep_high, sums[1], sums[0])
        sent = jnp.where(keep_high, sums[0], sums[1]).astype(jnp.bfloat16)
        summed = kept + permuted(sent, "col", 4).astype(jnp.float32)
        return (residual.astype(jnp.float32) + gelu_tanh(summed)).astype(jnp.bfloat16)

    def input_gradient(quad, upstream):
        slopes = jnp.moveaxis(quad, 0, 1).reshape(-1, tokens)
        parts = jnp.zeros((ROWS, width, tokens), jnp.bfloat16)
        for step, piece in enumerate(pieces):
            part = jnp.dot(piece, slopes, preferred_element_type=jnp.float32)
            parts = with_slot(parts, part.astype(jnp.bfloat16), row ^ step)
        parts = spread_row(parts).astype(jnp.float32)
        return (upstream.astype(jnp.float32) + jnp.sum(parts, axis=0)).astype(jnp.bfloat16)

    inputs = slot_of(acts, front)
    upstream = slot_of(grads, back)
    slope = slope_of(upstream, slot_of(saved, back))
    other = permuted(slope, "col", 4)
    later_inputs = slot_of(acts, later_front)
    later_upstream = slot_of(grads, later_back)
    later_stored = slot_of(saved, later_back)
    other, ends, keep_high, same_front, same_back, later_front = lax.optimization_barrier(
        (other, ends, keep_high, same_front, same_back, later_front)
    )
    later_inputs, later_upstream, later_stored, other = lax.optimization_barrier(
        (later_inputs, later_upstream, later_stored, other)
    )
    blocks = from_row(inputs)
    quad = spread_quad(quad_pieces(slope, other, upper))
    residual = jnp.where(ends, twisted(inputs), inputs)
    got = spread_quad(forward_sums(blocks))
    returned = relay(input_gradient(quad, upstream), -1)
    arrived = relay(layer_output(got, residual), 1)

    inputs = jnp.where(same_front, arrived, later_inputs)
    copies = jnp.broadcast_to(inputs[None], (ROWS, width, tokens))
    copies = spread_row(copies)
    blocks = [slot_of(copies, row ^ step) for step in range(ROWS)]
    residual = jnp.where(ends, twisted(inputs), inputs)
    upstream = jnp.where(same_back, returned, later_upstream)
    slope = slope_of(upstream, later_stored)
    other = permuted(slope, "col", 4)
    both = jnp.concatenate([forward_sums(blocks), quad_pieces(slope, other, upper)], axis=1)
    both = spread_quad(both)
    slots = jnp.arange(SLOTS)[:, None, None]
    held_inputs = jnp.where(slots == front, arrived, acts)
    held_grads = jnp.where(slots == back, returned, grads)
    returned = input_gradient(both[:, 2:], upstream)
    count = lax.axis_size("section")
    most = relay(returned, -1, range(1, count))
    wrapped = relay(returned, -1, (0,))
    returned = jnp.where(section == count - 1, wrapped, most)
    arrived = relay(layer_output(both[:, :2], residual), 1)
    held_inputs = jnp.where(slots == later_front, arrived, held_inputs)
    held_grads = jnp.where(slots == later_back, returned, held_grads)
    return (held_inputs[None], held_grads[None])


def solution(mesh):
    return jax.shard_map(
        shards,
        mesh=mesh,
        in_specs=(
            P("section", ("row", "col"), None),
            P("section", None, ("row", "col"), None),
            P("section", None, ("row", "col"), None),
            P("section", None, ("row", "col"), None),
            P("section", None, None),
        ),
        out_specs=(
            P("section", None, ("row", "col"), None),
            P("section", None, ("row", "col"), None),
        ),
        check_vma=False,
    )
```
